128 devices in a mesh: node: 32 (over x, z, core), local: 4 (over y).
Axes of the slice: x: 4, y: 4, z: 4, core: 2. Of those that a mesh axis runs over, the one named last changes fastest.
Arguments:
- tokens: bfloat16 [8192, 5120], P(('node', 'local')), may hold values from -6 to 6
- node_ids: int32 [8192, 3], P(('node', 'local')), may hold values from 0 to 31, as said below
- expert_ids: int32 [8192, 6], P(('node', 'local')), may hold values from 0 to 95, as said below
- gate_weights: bfloat16 [8192, 6], P(('node', 'local')), may hold values from 0.049804688 to 1
- up_weight: bfloat16 [96, 5120, 1536], P('node', None, 'local'), may hold values from -0.078125 to 0.078125
- down_weight: bfloat16 [96, 1536, 5120], P('node', 'local'), may hold values from -0.15625 to 0.15625
Outputs:
- routed_out: bfloat16 [8192, 5120], P(('node', 'local'))
The draws below stay inside these ranges and needn't reach their ends.
Inputs may be any that keep to these rules, and one draw needn't show every extreme that they name: `node_ids`: each token names 3 different nodes; the 64 tokens of one device name every node exactly 6 times. Node m holds experts 3 * m to 3 * m + 2. For each j, expert_ids[t, 2 * j] and expert_ids[t, 2 * j + 1] are two different experts of node node_ids[t, j].
All inputs are finite; a program needn't handle non-finite values.
Results may differ from the reference program's by a relative error of at most 0.012.
Values may be sent and summed in bfloat16 or wider, within the bound.
No kernel may reach another device: no remote copies, remote signals or barrier semaphores. Data moves between devices by JAX's collectives and lax.ppermute only.
A program may use at most 192 MiB of HBM per device.

```python
import math
import jax
import jax.numpy as jnp
from jax import lax

D = 5120
FF = 1536
EXP_NODE = 3
TOPK = 6
NODES_SEL = 3
TOK_DEV = 64
TOKENS = 8192
EXPERTS = 96
CAP = 6
N_NODE = 32
N_LOCAL = 4


def routing_tables(key):
    blocks_total = TOKENS // TOK_DEV
    node_total = EXPERTS // EXP_NODE
    base_key = jax.random.fold_in(key, 11)

    def one_block(block_key):
        key_order, key_tokens, key_skip = jax.random.split(block_key, 3)
        node_order = jax.random.permutation(key_order, node_total).astype(jnp.int32)
        cycled = node_order[jnp.arange(NODES_SEL * TOK_DEV, dtype=jnp.int32) % node_total]
        triples = cycled.reshape(TOK_DEV, NODES_SEL)
        shuffled = triples[jax.random.permutation(key_tokens, TOK_DEV)]
        skipped = jax.random.randint(key_skip, (TOK_DEV, NODES_SEL), 0, EXP_NODE).astype(jnp.int32)
        return (shuffled, skipped)
    node_table, skip_table = jax.vmap(one_block)(jax.random.split(base_key, blocks_total))
    return (node_table.reshape(TOKENS, NODES_SEL), skip_table.reshape(TOKENS, NODES_SEL))


def draw_node_ids(key, part):
    node_table, skip_table = routing_tables(key)
    return node_table.astype(jnp.int32)


def draw_expert_ids(key, part):
    node_table, skip_table = routing_tables(key)
    first_pick = (skip_table + 1) % EXP_NODE
    second = (skip_table + 2) % EXP_NODE
    paired = jnp.stack([node_table * EXP_NODE + first_pick, node_table * EXP_NODE + second], axis=2)
    return paired.reshape(TOKENS, TOPK).astype(jnp.int32)


def shard_levels(stream_key, extent, cuts, low, largest):
    loudness = 1.0
    for axis_at, parts in cuts:
        heights = jax.random.uniform(jax.random.fold_in(jax.random.fold_in(stream_key, 6), axis_at), (parts,), jnp.float32, low / len(cuts), largest / len(cuts))
        loudness = loudness * jnp.repeat(jnp.exp(heights), extent[axis_at] // parts).reshape((-1,) + (1,) * (len(extent) - 1 - axis_at))
    return loudness


def bell_draw(key, dims, width, bound, pieces=(), kind=jnp.bfloat16):
    factor_of = shard_levels(key, dims, pieces, -0.22, 0.18) if pieces else 1.0
    values = jax.random.normal(key, dims, jnp.float32) * width * factor_of
    return jnp.minimum(jnp.maximum(values, -bound), bound).astype(kind)


def setup_inputs(seed: int = 0) -> dict:
    key_list = jax.random.split(jax.random.key(seed), 7)
    return {
        "tokens": bell_draw(key_list[0], (TOKENS, D), 1.0, 6.0, ((0, 128),)),
        "node_ids": draw_node_ids(jax.random.fold_in(key_list[6], 71), 0),
        "expert_ids": draw_expert_ids(jax.random.fold_in(key_list[6], 71), 0),
        "gate_weights": jnp.clip(jnp.exp(math.log(1.0) - 2.9996462 * jax.random.uniform(key_list[3], (TOKENS, TOPK), jnp.float32) ** shard_levels(key_list[3], (TOKENS, TOPK), ((0, 128),), -0.2, 0.2)), 0.049804688, 1.0).astype(jnp.bfloat16),
        "up_weight": bell_draw(key_list[4], (EXPERTS, D, FF), D ** -0.5, 0.078125, ((0, 32), (2, 4))),
        "down_weight": bell_draw(key_list[5], (EXPERTS, FF, D), FF ** -0.5, 0.15625, ((0, 32), (1, 4))),
    }


def reference(tokens, node_ids, expert_ids, gate_weights, up_weight, down_weight):
    row_total = N_NODE * N_LOCAL * CAP
    shard_size = FF // N_LOCAL

    def per_node(running, node_id):
        chosen = jnp.any(node_ids == node_id, axis=1)
        row_index = jnp.nonzero(chosen, size=row_total, fill_value=0)[0].astype(jnp.int32)
        picked = tokens[row_index]
        row_experts = expert_ids[row_index]
        row_gates = gate_weights[row_index].astype(jnp.float32)
        contrib = jnp.zeros((row_total, D), jnp.float32)
        for shard_index in range(N_LOCAL):
            partial_value = jnp.zeros((row_total, D), jnp.float32)
            for expert_slot in range(EXP_NODE):
                expert = node_id * EXP_NODE + expert_slot
                weight = jnp.sum(jnp.where(row_experts == expert, row_gates, jnp.float32(0.0)), axis=1)
                up_full = lax.dynamic_index_in_dim(up_weight, expert, 0, keepdims=False)
                down_full = lax.dynamic_index_in_dim(down_weight, expert, 0, keepdims=False)
                up_slice = up_full[:, shard_index * shard_size:(shard_index + 1) * shard_size]
                down_slice = down_full[shard_index * shard_size:(shard_index + 1) * shard_size, :]
                lifted = jnp.dot(picked, up_slice, preferred_element_type=jnp.float32)
                scaled = (jax.nn.silu(lifted) * weight[:, None]).astype(jnp.bfloat16)
                partial_value = partial_value + jnp.dot(scaled, down_slice, preferred_element_type=jnp.float32)
            contrib = contrib + partial_value.astype(jnp.bfloat16).astype(jnp.float32)
        running = running.at[row_index].add(contrib.astype(jnp.bfloat16).astype(jnp.float32))
        return running, None

    final_sum, unused = lax.scan(per_node, jnp.zeros((TOKENS, D), jnp.float32), jnp.arange(N_NODE, dtype=jnp.int32))
    return final_sum.astype(jnp.bfloat16)
```

```python
import functools

import jax
import jax.numpy as jnp
from jax import lax
from jax.experimental import pallas as pl
from jax.experimental.pallas import tpu as pltpu
from jax.sharding import PartitionSpec as P


GROUPS = 2
TAIL = 256
STEPS = 4
SMALL = pltpu.CompilerParams(vmem_limit_bytes=16 * 2**20)
LARGE = pltpu.CompilerParams(vmem_limit_bytes=44 * 2**20)
BF = jnp.bfloat16
F32 = jnp.float32


def nt_dot(a, b):
    return lax.dot_general(a, b, (((1,), (1,)), ((), ())), preferred_element_type=F32)


def select_kernel(nodes, group_ranks, per_node, node_ref, expert_ref, gate_ref, tok_ref, *outs):
    place_ref, group_refs = outs[0], outs[1:]
    tok_rows, width = tok_ref.shape
    slots = place_ref.shape[0]
    group_rows = nodes * group_ranks
    ids = node_ref[...]
    grid = lax.broadcasted_iota(jnp.int32, (nodes, tok_rows), 0)
    picked = jnp.zeros((nodes, tok_rows), F32)
    for j in range(ids.shape[0]):
        picked = picked + jnp.where(ids[j : j + 1, :] == grid, 1.0, 0.0)
    before = jnp.where(
        lax.broadcasted_iota(jnp.int32, (tok_rows, tok_rows), 0)
        < lax.broadcasted_iota(jnp.int32, (tok_rows, tok_rows), 1),
        1.0,
        0.0,
    ).astype(BF)
    rank = jnp.dot(picked.astype(BF), before, preferred_element_type=F32)
    rank = jnp.where(picked > 0.5, rank, -1.0).astype(BF)
    slot = lax.broadcasted_iota(jnp.int32, (slots, nodes), 0)
    owner = lax.rem(slot, group_rows) // group_ranks
    spread = jnp.where(
        owner == lax.broadcasted_iota(jnp.int32, (slots, nodes), 1), 1.0, 0.0
    ).astype(BF)
    slot_col = lax.broadcasted_iota(jnp.int32, (slots, 1), 0)
    want = (slot_col // group_rows) * group_ranks + lax.rem(slot_col, group_ranks)
    place = jnp.where(
        jnp.dot(spread, rank, preferred_element_type=F32) == want.astype(F32), 1.0, 0.0
    ).astype(BF)
    place_ref[...] = place
    ids_slot = nt_dot(place, expert_ref[...].astype(F32).astype(BF))
    gates_slot = nt_dot(place, gate_ref[...])
    base = ((lax.rem(slot_col, group_rows) // group_ranks) * per_node).astype(F32)
    lane = lax.broadcasted_iota(jnp.int32, (slots, TAIL), 1)
    tail = jnp.zeros((slots, TAIL), F32)
    for e in range(per_node):
        gate = jnp.sum(jnp.where(ids_slot == base + float(e), gates_slot, 0.0), axis=1, keepdims=True)
        tail = jnp.where(lane == e, gate, tail)
    tail = tail.astype(BF)
    for g, ref in enumerate(group_refs):
        rows = slice(g * group_rows, (g + 1) * group_rows)
        ref[:, width:] = tail[rows]
        ref[:, :width] = jnp.dot(place[rows], tok_ref[...], preferred_element_type=F32).astype(BF)


def select(tokens, node_ids, expert_ids, gate_weights, nodes, per_node):
    tok_rows, width = tokens.shape
    slots = tok_rows * node_ids.shape[1]
    capacity = slots // nodes
    ranks = capacity // GROUPS
    vm = pl.BlockSpec(memory_space=pltpu.VMEM)
    return pl.pallas_call(
        functools.partial(select_kernel, nodes, ranks, per_node),
        out_shape=[jax.ShapeDtypeStruct((slots, tok_rows), BF)]
        + [jax.ShapeDtypeStruct((nodes * ranks, width + TAIL), BF)] * GROUPS,
        in_specs=[vm] * 4,
        out_specs=[vm] * (GROUPS + 1),
        compiler_params=SMALL,
        name="select",
    )(node_ids.T, expert_ids.T, gate_weights.T, tokens)


def up_kernel(own, right, left, far_a, far_b, up, hid, x, acc):
    step = pl.program_id(0)
    width = x.shape[1] - TAIL
    chunk = width // STEPS
    per_node, _, part = up.shape

    @pl.when(step == 0)
    def _():
        at = 0
        for p in (own, right, left, far_a, far_b):
            x[at : at + p.shape[0], :] = p[...]
            at += p.shape[0]

    cols = x[:, pl.ds(pl.multiple_of(step * chunk, 128), chunk)]
    weight = jnp.concatenate([up[e] for e in range(per_node)], axis=1)
    value = jnp.dot(cols, weight, preferred_element_type=F32)

    @pl.when(step == 0)
    def _():
        acc[...] = value

    @pl.when(step > 0)
    def _():
        acc[...] += value

    @pl.when(step == STEPS - 1)
    def _():
        gates = x[:, width:].astype(F32)
        for e in range(per_node):
            piece = slice(e * part, (e + 1) * part)
            v = acc[:, piece]
            hid[:, piece] = (v / (1.0 + jnp.exp(-v)) * gates[:, e : e + 1]).astype(BF)


def cost(rows, width, units):
    return pl.CostEstimate(
        flops=2 * rows * width * units,
        transcendentals=0,
        bytes_accessed=2 * (width * units + rows * width + rows * units),
    )


def up_project(parts, up):
    per_node, width, part = up.shape
    units = per_node * part
    rows = sum(p.shape[0] for p in parts)
    return pl.pallas_call(
        up_kernel,
        grid=(STEPS,),
        out_shape=jax.ShapeDtypeStruct((rows, units), BF),
        in_specs=[pl.BlockSpec(p.shape, lambda i: (0, 0)) for p in parts]
        + [pl.BlockSpec((per_node, width // STEPS, part), lambda i: (0, i, 0))],
        out_specs=pl.BlockSpec((rows, units), lambda i: (0, 0)),
        scratch_shapes=[pltpu.VMEM((rows, width + TAIL), BF), pltpu.VMEM((rows, units), F32)],
        compiler_params=LARGE,
        cost_estimate=cost(rows, width, units),
        name="up",
    )(*parts, up)


def down_kernel(hid, down, *outs):
    per_node, part, chunk = down.shape
    weight = down[...].reshape(per_node * part, chunk)
    value = jnp.dot(hid[...], weight, preferred_element_type=F32).astype(BF)
    at = 0
    for o in outs:
        o[...] = value[at : at + o.shape[0]]
        at += o.shape[0]


def down_project(hid, down, sizes):
    per_node, part, width = down.shape
    rows, units = hid.shape
    chunk = width // STEPS
    return pl.pallas_call(
        down_kernel,
        grid=(STEPS,),
        out_shape=[jax.ShapeDtypeStruct((s, width), BF) for s in sizes],
        in_specs=[
            pl.BlockSpec((rows, units), lambda i: (0, 0)),
            pl.BlockSpec((per_node, part, chunk), lambda i: (0, 0, i)),
        ],
        out_specs=[pl.BlockSpec((s, chunk), lambda i: (0, i)) for s in sizes],
        compiler_params=LARGE,
        cost_estimate=cost(rows, width, units),
        name="down",
    )(hid, down)


def shift(value, by):
    size = lax.axis_size("local")
    return lax.ppermute(value, "local", [(i, (i + by) % size) for i in range(size)])


def to_nodes(value, nodes):
    rows, width = value.shape
    pieces = value.reshape(nodes, rows // nodes, 2, width // 2)
    swapped = lax.all_to_all(pieces, "node", split_axis=0, concat_axis=0, tiled=True)
    return swapped.reshape(rows, width)


def add(*values):
    total = values[0].astype(F32)
    for v in values[1:]:
        total = total + v.astype(F32)
    return total.astype(BF)


def body(tokens, node_ids, expert_ids, gate_weights, up_weight, down_weight):
    nodes = lax.axis_size("node")
    place, *groups = select(
        tokens, node_ids, expert_ids, gate_weights, nodes, up_weight.shape[0]
    )
    half = groups[0].shape[0] // 2
    gathered = []
    for sent in groups:
        own = to_nodes(sent, nodes)
        right, left = shift(own, 1), shift(own, -1)
        far_a, far_b = shift(right[:half], 1), shift(left[half:], -1)
        gathered.append((own, right, left, far_a, far_b))
    returned = []
    for g, parts in enumerate(gathered):
        hid = up_project(parts, up_weight)
        own, right, left, far_a, far_b = down_project(hid, down_weight, [p.shape[0] for p in parts])
        in_a, in_b = shift(far_a, 1), shift(far_b, -1)
        late_left, late_right = left[half:], right[:half]
        if g == len(gathered) - 1:
            late_left, late_right = shift(late_left, 1), shift(late_right, -1)
            soon_left = shift(add(left[:half], in_a), 1)
            soon_right = shift(add(right[half:], in_b), -1)
            total = jnp.concatenate(
                [add(own[:half], soon_left, late_right), add(own[half:], late_left, soon_right)],
                axis=0,
            )
        else:
            left = jnp.concatenate([add(left[:half], in_a), late_left], axis=0)
            right = jnp.concatenate([late_right, add(right[half:], in_b)], axis=0)
            total = add(own, shift(left, 1), shift(right, -1))
        returned.append(to_nodes(total, nodes))
    combined = lax.dot_general(
        place,
        jnp.concatenate(returned, axis=0),
        (((0,), (0,)), ((), ())),
        preferred_element_type=F32,
    )
    return combined.astype(BF)


def solution(mesh):
    in_specs = (
        P(("node", "local"), None),
        P(("node", "local"), None),
        P(("node", "local"), None),
        P(("node", "local"), None),
        P("node", None, "local"),
        P("node", "local", None),
    )
    out_specs = P(("node", "local"), None)

    return jax.shard_map(body, mesh=mesh, in_specs=in_specs, out_specs=out_specs, check_vma=False)
```

```python
import functools

import jax
import jax.numpy as jnp
from jax import lax
from jax.experimental import pallas as pl
from jax.experimental.pallas import tpu as pltpu
from jax.sharding import PartitionSpec as P


GROUPS = 2
TAIL = 256
LANES = 128
STEPS = 4
SMALL = pltpu.CompilerParams(vmem_limit_bytes=16 * 2**20)
LARGE = pltpu.CompilerParams(vmem_limit_bytes=44 * 2**20)
BF = jnp.bfloat16
F32 = jnp.float32


def nt_dot(a, b):
    return lax.dot_general(a, b, (((1,), (1,)), ((), ())), preferred_element_type=F32)


def select_kernel(nodes, group_ranks, per_node, *refs):
    sources, outs, copies, sems = refs[:4], refs[4 : 5 + GROUPS], refs[5 + GROUPS : -1], refs[-1]
    moves = [
        pltpu.make_async_copy(s, c, sems.at[i]) for i, (s, c) in enumerate(zip(sources, copies))
    ]
    for m in moves:
        m.start()
    for m in moves:
        m.wait()
    node_ref, expert_ref, gate_ref, tok_ref = copies
    place_ref, group_refs = outs[0], outs[1:]
    tok_rows, width = tok_ref.shape
    slots = place_ref.shape[0]
    group_rows = nodes * group_ranks
    ids = node_ref[...]
    grid = lax.broadcasted_iota(jnp.int32, (nodes, tok_rows), 0)
    picked = jnp.zeros((nodes, tok_rows), F32)
    for j in range(ids.shape[0]):
        picked = picked + jnp.where(ids[j : j + 1, :] == grid, 1.0, 0.0)
    before = jnp.where(
        lax.broadcasted_iota(jnp.int32, (tok_rows, tok_rows), 0)
        < lax.broadcasted_iota(jnp.int32, (tok_rows, tok_rows), 1),
        1.0,
        0.0,
    ).astype(BF)
    rank = jnp.dot(picked.astype(BF), before, preferred_element_type=F32)
    rank = jnp.where(picked > 0.5, rank, -1.0).astype(BF)
    slot = lax.broadcasted_iota(jnp.int32, (slots, nodes), 0)
    owner = lax.rem(slot, group_rows) // group_ranks
    spread = jnp.where(
        owner == lax.broadcasted_iota(jnp.int32, (slots, nodes), 1), 1.0, 0.0
    ).astype(BF)
    slot_col = lax.broadcasted_iota(jnp.int32, (slots, 1), 0)
    want = (slot_col // group_rows) * group_ranks + lax.rem(slot_col, group_ranks)
    place = jnp.where(
        jnp.dot(spread, rank, preferred_element_type=F32) == want.astype(F32), 1.0, 0.0
    ).astype(BF)
    place_ref[...] = place
    ids_slot = nt_dot(place, expert_ref[...].astype(F32).astype(BF))
    gates_slot = nt_dot(place, gate_ref[...])
    base = ((lax.rem(slot_col, group_rows) // group_ranks) * per_node).astype(F32)
    lane = lax.broadcasted_iota(jnp.int32, (group_rows, TAIL), 1)
    tail = jnp.zeros((group_rows, TAIL), F32)
    for e in range(per_node):
        gate = jnp.sum(jnp.where(ids_slot == base + float(e), gates_slot, 0.0), axis=1, keepdims=True)
        for g in range(GROUPS):
            rows = slice(g * group_rows, (g + 1) * group_rows)
            tail = jnp.where(lane == g * per_node + e, gate[rows], tail)
    group_refs[0][:, width:] = tail.astype(BF)
    for g, ref in enumerate(group_refs):
        rows = slice(g * group_rows, (g + 1) * group_rows)
        ref[:, :width] = jnp.dot(place[rows], tok_ref[...], preferred_element_type=F32).astype(BF)


def select(tokens, node_ids, expert_ids, gate_weights, nodes, per_node):
    tok_rows, width = tokens.shape
    slots = tok_rows * node_ids.shape[1]
    capacity = slots // nodes
    ranks = capacity // GROUPS
    vm = pl.BlockSpec(memory_space=pltpu.VMEM)
    operands = (node_ids.T, expert_ids.T, gate_weights.T, tokens)
    return pl.pallas_call(
        functools.partial(select_kernel, nodes, ranks, per_node),
        out_shape=[jax.ShapeDtypeStruct((slots, tok_rows), BF)]
        + [
            jax.ShapeDtypeStruct((nodes * ranks, width + (TAIL if g == 0 else 0)), BF)
            for g in range(GROUPS)
        ],
        in_specs=[pl.BlockSpec(memory_space=pltpu.HBM)] * 4,
        out_specs=[vm] * (GROUPS + 1),
        scratch_shapes=[pltpu.VMEM(v.shape, v.dtype) for v in operands]
        + [pltpu.SemaphoreType.DMA((len(operands),))],
        compiler_params=SMALL,
        name="select",
    )(*operands)


def up_kernel(parts, gate_parts, first_gate, *refs):
    xs, gate_refs = refs[:parts], refs[parts : parts + gate_parts]
    up, hid, x, acc = refs[parts + gate_parts :]
    step = pl.program_id(0)
    chunk = x.shape[1] // STEPS
    per_node, _, part = up.shape

    @pl.when(step == 0)
    def _():
        at = 0
        for p in xs:
            x[at : at + p.shape[0], :] = p[:, : x.shape[1]]
            at += p.shape[0]

    cols = x[:, pl.ds(pl.multiple_of(step * chunk, 128), chunk)]
    weight = jnp.concatenate([up[e] for e in range(per_node)], axis=1)
    value = jnp.dot(cols, weight, preferred_element_type=F32)

    @pl.when(step == 0)
    def _():
        acc[...] = value

    @pl.when(step > 0)
    def _():
        acc[...] += value

    @pl.when(step == STEPS - 1)
    def _():
        gates = jnp.concatenate([r[...] for r in gate_refs], axis=0).astype(F32)
        for e in range(per_node):
            piece = slice(e * part, (e + 1) * part)
            v = acc[:, piece]
            hid[:, piece] = (v / (1.0 + jnp.exp(-v)) * gates[:, first_gate + e : first_gate + e + 1]).astype(BF)


def cost(rows, width, units):
    return pl.CostEstimate(
        flops=2 * rows * width * units,
        transcendentals=0,
        bytes_accessed=2 * (width * units + rows * width + rows * units),
    )


def up_project(parts, gate_parts, first_gate, up):
    per_node, width, part = up.shape
    units = per_node * part
    rows = sum(p.shape[0] for p in parts)
    return pl.pallas_call(
        functools.partial(up_kernel, len(parts), len(gate_parts), first_gate),
        grid=(STEPS,),
        out_shape=jax.ShapeDtypeStruct((rows, units), BF),
        in_specs=[pl.BlockSpec(p.shape, lambda i: (0, 0)) for p in parts]
        + [pl.BlockSpec((p.shape[0], LANES), lambda i: (0, width // LANES)) for p in gate_parts]
        + [pl.BlockSpec((per_node, width // STEPS, part), lambda i: (0, i, 0))],
        out_specs=pl.BlockSpec((rows, units), lambda i: (0, 0)),
        scratch_shapes=[pltpu.VMEM((rows, width), BF), pltpu.VMEM((rows, units), F32)],
        compiler_params=LARGE,
        cost_estimate=cost(rows, width, units),
        name="up",
    )(*parts, *gate_parts, up)


def down_kernel(hid, down, *outs):
    per_node, part, chunk = down.shape
    weight = down[...].reshape(per_node * part, chunk)
    value = jnp.dot(hid[...], weight, preferred_element_type=F32).astype(BF)
    at = 0
    for o in outs:
        o[...] = value[at : at + o.shape[0]]
        at += o.shape[0]


def down_project(hid, down, sizes):
    per_node, part, width = down.shape
    rows, units = hid.shape
    chunk = width // STEPS
    return pl.pallas_call(
        down_kernel,
        grid=(STEPS,),
        out_shape=[jax.ShapeDtypeStruct((s, width), BF) for s in sizes],
        in_specs=[
            pl.BlockSpec((rows, units), lambda i: (0, 0)),
            pl.BlockSpec((per_node, part, chunk), lambda i: (0, 0, i)),
        ],
        out_specs=[pl.BlockSpec((s, chunk), lambda i: (0, i)) for s in sizes],
        compiler_params=LARGE,
        cost_estimate=cost(rows, width, units),
        name="down",
    )(hid, down)


def shift(value, by):
    size = lax.axis_size("local")
    return lax.ppermute(value, "local", [(i, (i + by) % size) for i in range(size)])


def to_nodes(value, nodes):
    rows, width = value.shape
    pieces = value.reshape(nodes, rows // nodes, 2, width // 2)
    swapped = lax.all_to_all(pieces, "node", split_axis=0, concat_axis=0, tiled=True)
    return swapped.reshape(rows, width)


def add(*values):
    total = values[0].astype(F32)
    for v in values[1:]:
        total = total + v.astype(F32)
    return total.astype(BF)


def body(tokens, node_ids, expert_ids, gate_weights, up_weight, down_weight):
    nodes = lax.axis_size("node")
    place, *groups = select(
        tokens, node_ids, expert_ids, gate_weights, nodes, up_weight.shape[0]
    )
    half = groups[0].shape[0] // 2
    gathered = []
    for g, sent in enumerate(groups):
        own = to_nodes(sent, nodes)
        if g == 0:
            top, low = own[:half], own[half:]
            right_top, left_low = shift(top, 1), shift(low, -1)
            right_low, left_top = shift(low, 1), shift(top, -1)
            far_a, far_b = shift(right_top, 1), shift(left_low, -1)
            parts = (top, low, right_top, right_low, left_top, left_low, far_a, far_b)
        else:
            right, left = shift(own, 1), shift(own, -1)
            far_a, far_b = shift(right[:half], 1), shift(left[half:], -1)
            parts = (own, right, left, far_a, far_b)
        gathered.append(parts)
    returned = []
    for g, parts in enumerate(gathered):
        hid = up_project(parts, gathered[0], g * up_weight.shape[0], up_weight)
        own, right, left, far_a, far_b = down_project(hid, down_weight, [2 * half] * 3 + [half] * 2)
        in_a, in_b = shift(far_a, 1), shift(far_b, -1)
        late_left, late_right = left[half:], right[:half]
        if g == len(gathered) - 1:
            late_left, late_right = shift(late_left, 1), shift(late_right, -1)
            soon_left = shift(add(left[:half], in_a), 1)
            soon_right = shift(add(right[half:], in_b), -1)
            total = jnp.concatenate(
                [add(own[:half], soon_left, late_right), add(own[half:], late_left, soon_right)],
                axis=0,
            )
        else:
            left = jnp.concatenate([add(left[:half], in_a), late_left], axis=0)
            right = jnp.concatenate([late_right, add(right[half:], in_b)], axis=0)
            total = add(own, shift(left, 1), shift(right, -1))
        returned.append(to_nodes(total, nodes))
    combined = lax.dot_general(
        place,
        jnp.concatenate(returned, axis=0),
        (((0,), (0,)), ((), ())),
        preferred_element_type=F32,
    )
    return combined.astype(BF)


def solution(mesh):
    in_specs = (
        P(("node", "local"), None),
        P(("node", "local"), None),
        P(("node", "local"), None),
        P(("node", "local"), None),
        P("node", None, "local"),
        P("node", "local", None),
    )
    out_specs = P(("node", "local"), None)

    return jax.shard_map(body, mesh=mesh, in_specs=in_specs, out_specs=out_specs, check_vma=False)
```

```python
import functools

import jax
import jax.numpy as jnp
from jax import lax
from jax.experimental import pallas as pl
from jax.experimental.pallas import tpu as pltpu
from jax.sharding import PartitionSpec as P


GROUPS = 2
TAIL = 256
LANES = 128
STEPS = 4
SMALL = pltpu.CompilerParams(vmem_limit_bytes=16 * 2**20)
LARGE = pltpu.CompilerParams(vmem_limit_bytes=44 * 2**20)
BF = jnp.bfloat16
F32 = jnp.float32


def nt_dot(a, b):
    return lax.dot_general(a, b, (((1,), (1,)), ((), ())), preferred_element_type=F32)


def select_kernel(nodes, group_ranks, per_node, *refs):
    sources, outs, copies, sems = refs[:4], refs[4 : 5 + GROUPS], refs[5 + GROUPS : -1], refs[-1]
    moves = [
        pltpu.make_async_copy(s, c, sems.at[i]) for i, (s, c) in enumerate(zip(sources, copies))
    ]
    for m in moves:
        m.start()
    for m in moves:
        m.wait()
    node_ref, expert_ref, gate_ref, tok_ref = copies
    place_ref, group_refs = outs[0], outs[1:]
    tok_rows, width = tok_ref.shape
    slots = place_ref.shape[0]
    group_rows = nodes * group_ranks
    ids = node_ref[...]
    grid = lax.broadcasted_iota(jnp.int32, (nodes, tok_rows), 0)
    picked = jnp.zeros((nodes, tok_rows), F32)
    for j in range(ids.shape[0]):
        picked = picked + jnp.where(ids[j : j + 1, :] == grid, 1.0, 0.0)
    before = jnp.where(
        lax.broadcasted_iota(jnp.int32, (tok_rows, tok_rows), 0)
        < lax.broadcasted_iota(jnp.int32, (tok_rows, tok_rows), 1),
        1.0,
        0.0,
    ).astype(BF)
    rank = jnp.dot(picked.astype(BF), before, preferred_element_type=F32)
    rank = jnp.where(picked > 0.5, rank, -1.0).astype(BF)
    slot = lax.broadcasted_iota(jnp.int32, (slots, nodes), 0)
    owner = lax.rem(slot, group_rows) // group_ranks
    spread = jnp.where(
        owner == lax.broadcasted_iota(jnp.int32, (slots, nodes), 1), 1.0, 0.0
    ).astype(BF)
    slot_col = lax.broadcasted_iota(jnp.int32, (slots, 1), 0)
    want = (slot_col // group_rows) * group_ranks + lax.rem(slot_col, group_ranks)
    place = jnp.where(
        jnp.dot(spread, rank, preferred_element_type=F32) == want.astype(F32), 1.0, 0.0
    ).astype(BF)
    place_ref[...] = place
    ids_slot = nt_dot(place, expert_ref[...].astype(F32).astype(BF))
    gates_slot = nt_dot(place, gate_ref[...])
    base = ((lax.rem(slot_col, group_rows) // group_ranks) * per_node).astype(F32)
    lane = lax.broadcasted_iota(jnp.int32, (group_rows, TAIL), 1)
    tail = jnp.zeros((group_rows, TAIL), F32)
    for e in range(per_node):
        gate = jnp.sum(jnp.where(ids_slot == base + float(e), gates_slot, 0.0), axis=1, keepdims=True)
        for g in range(GROUPS):
            rows = slice(g * group_rows, (g + 1) * group_rows)
            tail = jnp.where(lane == g * per_node + e, gate[rows], tail)
    group_refs[0][:, width:] = tail.astype(BF)
    for g, ref in enumerate(group_refs):
        rows = slice(g * group_rows, (g + 1) * group_rows)
        ref[:, :width] = jnp.dot(place[rows], tok_ref[...], preferred_element_type=F32).astype(BF)


def select(tokens, node_ids, expert_ids, gate_weights, nodes, per_node):
    tok_rows, width = tokens.shape
    slots = tok_rows * node_ids.shape[1]
    capacity = slots // nodes
    ranks = capacity // GROUPS
    vm = pl.BlockSpec(memory_space=pltpu.VMEM)
    operands = (node_ids.T, expert_ids.T, gate_weights.T, tokens)
    return pl.pallas_call(
        functools.partial(select_kernel, nodes, ranks, per_node),
        out_shape=[jax.ShapeDtypeStruct((slots, tok_rows), BF)]
        + [
            jax.ShapeDtypeStruct((nodes * ranks, width + (TAIL if g == 0 else 0)), BF)
            for g in range(GROUPS)
        ],
        in_specs=[pl.BlockSpec(memory_space=pltpu.HBM)] * 4,
        out_specs=[vm] * (GROUPS + 1),
        scratch_shapes=[pltpu.VMEM(v.shape, v.dtype) for v in operands]
        + [pltpu.SemaphoreType.DMA((len(operands),))],
        compiler_params=SMALL,
        name="select",
    )(*operands)


def up_kernel(parts, gate_parts, first_gate, *refs):
    xs, gate_refs = refs[:parts], refs[parts : parts + gate_parts]
    up, hid, x, acc = refs[parts + gate_parts :]
    step = pl.program_id(0)
    chunk = x.shape[1] // STEPS
    per_node, _, part = up.shape

    @pl.when(step == 0)
    def _():
        at = 0
        for p in xs:
            x[at : at + p.shape[0], :] = p[:, : x.shape[1]]
            at += p.shape[0]

    cols = x[:, pl.ds(pl.multiple_of(step * chunk, 128), chunk)]
    weight = jnp.concatenate([up[e] for e in range(per_node)], axis=1)
    value = jnp.dot(cols, weight, preferred_element_type=F32)

    @pl.when(step == 0)
    def _():
        acc[...] = value

    @pl.when(step > 0)
    def _():
        acc[...] += value

    @pl.when(step == STEPS - 1)
    def _():
        gates = jnp.concatenate([r[...] for r in gate_refs], axis=0).astype(F32)
        for e in range(per_node):
            piece = slice(e * part, (e + 1) * part)
            v = acc[:, piece]
            hid[:, piece] = (v / (1.0 + jnp.exp(-v)) * gates[:, first_gate + e : first_gate + e + 1]).astype(BF)


def cost(rows, width, units):
    return pl.CostEstimate(
        flops=2 * rows * width * units,
        transcendentals=0,
        bytes_accessed=2 * (width * units + rows * width + rows * units),
    )


def up_project(parts, gate_parts, first_gate, up):
    per_node, width, part = up.shape
    units = per_node * part
    rows = sum(p.shape[0] for p in parts)
    return pl.pallas_call(
        functools.partial(up_kernel, len(parts), len(gate_parts), first_gate),
        grid=(STEPS,),
        out_shape=jax.ShapeDtypeStruct((rows, units), BF),
        in_specs=[pl.BlockSpec(p.shape, lambda i: (0, 0)) for p in parts]
        + [pl.BlockSpec((p.shape[0], LANES), lambda i: (0, width // LANES)) for p in gate_parts]
        + [pl.BlockSpec((per_node, width // STEPS, part), lambda i: (0, i, 0))],
        out_specs=pl.BlockSpec((rows, units), lambda i: (0, 0)),
        scratch_shapes=[pltpu.VMEM((rows, width), BF), pltpu.VMEM((rows, units), F32)],
        compiler_params=LARGE,
        cost_estimate=cost(rows, width, units),
        name="up",
    )(*parts, *gate_parts, up)


def down_kernel(hid, down, *outs):
    per_node, part, chunk = down.shape
    weight = down[...].reshape(per_node * part, chunk)
    value = jnp.dot(hid[...], weight, preferred_element_type=F32).astype(BF)
    at = 0
    for o in outs:
        o[...] = value[at : at + o.shape[0]]
        at += o.shape[0]


def down_project(hid, down, sizes):
    per_node, part, width = down.shape
    rows, units = hid.shape
    chunk = width // STEPS
    return pl.pallas_call(
        down_kernel,
        grid=(STEPS,),
        out_shape=[jax.ShapeDtypeStruct((s, width), BF) for s in sizes],
        in_specs=[
            pl.BlockSpec((rows, units), lambda i: (0, 0)),
            pl.BlockSpec((per_node, part, chunk), lambda i: (0, 0, i)),
        ],
        out_specs=[pl.BlockSpec((s, chunk), lambda i: (0, i)) for s in sizes],
        compiler_params=LARGE,
        cost_estimate=cost(rows, width, units),
        name="down",
    )(hid, down)


def shift(value, by):
    size = lax.axis_size("local")
    return lax.ppermute(value, "local", [(i, (i + by) % size) for i in range(size)])


def to_nodes(value, nodes):
    rows, width = value.shape
    pieces = value.reshape(nodes, rows // nodes, 2, width // 2)
    swapped = lax.all_to_all(pieces, "node", split_axis=0, concat_axis=0, tiled=True)
    return swapped.reshape(rows, width)


def add(*values):
    total = values[0].astype(F32)
    for v in values[1:]:
        total = total + v.astype(F32)
    return total.astype(BF)


def body(tokens, node_ids, expert_ids, gate_weights, up_weight, down_weight):
    nodes = lax.axis_size("node")
    place, *groups = select(
        tokens, node_ids, expert_ids, gate_weights, nodes, up_weight.shape[0]
    )
    half = groups[0].shape[0] // 2
    gathered = []
    for sent in groups:
        own = to_nodes(sent, nodes)
        top, low = own[:half], own[half:]
        right_top, left_low = shift(top, 1), shift(low, -1)
        right_low, left_top = shift(low, 1), shift(top, -1)
        far_a, far_b = shift(right_top, 1), shift(left_low, -1)
        parts = (top, low, right_top, right_low, left_top, left_low, far_a, far_b)
        gathered.append(parts)
    returned = []
    for g, parts in enumerate(gathered):
        hid = up_project(parts, gathered[0], g * up_weight.shape[0], up_weight)
        own, right, left, far_a, far_b = down_project(hid, down_weight, [2 * half] * 3 + [half] * 2)
        in_a, in_b = shift(far_a, 1), shift(far_b, -1)
        late_left, late_right = shift(left[half:], 1), shift(right[:half], -1)
        soon_left = shift(add(left[:half], in_a), 1)
        soon_right = shift(add(right[half:], in_b), -1)
        total = jnp.concatenate(
            [add(own[:half], soon_left, late_right), add(own[half:], late_left, soon_right)], axis=0
        )
        returned.append(to_nodes(total, nodes))
    combined = lax.dot_general(
        place,
        jnp.concatenate(returned, axis=0),
        (((0,), (0,)), ((), ())),
        preferred_element_type=F32,
    )
    return combined.astype(BF)


def solution(mesh):
    in_specs = (
        P(("node", "local"), None),
        P(("node", "local"), None),
        P(("node", "local"), None),
        P(("node", "local"), None),
        P("node", None, "local"),
        P("node", "local", None),
    )
    out_specs = P(("node", "local"), None)

    return jax.shard_map(body, mesh=mesh, in_specs=in_specs, out_specs=out_specs, check_vma=False)
```

```python
import functools

import jax
import jax.numpy as jnp
from jax import lax
from jax.experimental import pallas as pl
from jax.experimental.pallas import tpu as pltpu
from jax.sharding import PartitionSpec as P


GROUPS = 2
TAIL = 256
LANES = 128
STEPS = 4
SMALL = pltpu.CompilerParams(vmem_limit_bytes=16 * 2**20)
LARGE = pltpu.CompilerParams(vmem_limit_bytes=44 * 2**20)
BF = jnp.bfloat16
F32 = jnp.float32


def nt_dot(a, b):
    return lax.dot_general(a, b, (((1,), (1,)), ((), ())), preferred_element_type=F32)


def select_kernel(nodes, group_ranks, per_node, *refs):
    sources, outs, copies, sems = refs[:4], refs[4 : 5 + GROUPS], refs[5 + GROUPS : -1], refs[-1]
    moves = [
        pltpu.make_async_copy(s, c, sems.at[i]) for i, (s, c) in enumerate(zip(sources, copies))
    ]
    for m in moves:
        m.start()
    for m in moves:
        m.wait()
    node_ref, expert_ref, gate_ref, tok_ref = copies
    place_ref, group_refs = outs[0], outs[1:]
    tok_rows, width = tok_ref.shape
    slots = place_ref.shape[0]
    group_rows = nodes * group_ranks
    ids = node_ref[...]
    grid = lax.broadcasted_iota(jnp.int32, (nodes, tok_rows), 0)
    picked = jnp.zeros((nodes, tok_rows), F32)
    for j in range(ids.shape[0]):
        picked = picked + jnp.where(ids[j : j + 1, :] == grid, 1.0, 0.0)
    before = jnp.where(
        lax.broadcasted_iota(jnp.int32, (tok_rows, tok_rows), 0)
        < lax.broadcasted_iota(jnp.int32, (tok_rows, tok_rows), 1),
        1.0,
        0.0,
    ).astype(BF)
    rank = jnp.dot(picked.astype(BF), before, preferred_element_type=F32)
    rank = jnp.where(picked > 0.5, rank, -1.0).astype(BF)
    slot = lax.broadcasted_iota(jnp.int32, (slots, nodes), 0)
    owner = lax.rem(slot, group_rows) // group_ranks
    spread = jnp.where(
        owner == lax.broadcasted_iota(jnp.int32, (slots, nodes), 1), 1.0, 0.0
    ).astype(BF)
    slot_col = lax.broadcasted_iota(jnp.int32, (slots, 1), 0)
    want = (slot_col // group_rows) * group_ranks + lax.rem(slot_col, group_ranks)
    place = jnp.where(
        jnp.dot(spread, rank, preferred_element_type=F32) == want.astype(F32), 1.0, 0.0
    ).astype(BF)
    place_ref[...] = place
    ids_slot = nt_dot(place, expert_ref[...].astype(F32).astype(BF))
    gates_slot = nt_dot(place, gate_ref[...])
    base = ((lax.rem(slot_col, group_rows) // group_ranks) * per_node).astype(F32)
    lane = lax.broadcasted_iota(jnp.int32, (group_rows, TAIL), 1)
    tail = jnp.zeros((group_rows, TAIL), F32)
    for e in range(per_node):
        gate = jnp.sum(jnp.where(ids_slot == base + float(e), gates_slot, 0.0), axis=1, keepdims=True)
        for g in range(GROUPS):
            rows = slice(g * group_rows, (g + 1) * group_rows)
            tail = jnp.where(lane == g * per_node + e, gate[rows], tail)
    group_refs[0][:, width:] = tail.astype(BF)
    for g, ref in enumerate(group_refs):
        rows = slice(g * group_rows, (g + 1) * group_rows)
        ref[:, :width] = jnp.dot(place[rows], tok_ref[...], preferred_element_type=F32).astype(BF)


def select(tokens, node_ids, expert_ids, gate_weights, nodes, per_node):
    tok_rows, width = tokens.shape
    slots = tok_rows * node_ids.shape[1]
    capacity = slots // nodes
    ranks = capacity // GROUPS
    vm = pl.BlockSpec(memory_space=pltpu.VMEM)
    operands = (node_ids.T, expert_ids.T, gate_weights.T, tokens)
    return pl.pallas_call(
        functools.partial(select_kernel, nodes, ranks, per_node),
        out_shape=[jax.ShapeDtypeStruct((slots, tok_rows), BF)]
        + [
            jax.ShapeDtypeStruct((nodes * ranks, width + (TAIL if g == 0 else 0)), BF)
            for g in range(GROUPS)
        ],
        in_specs=[pl.BlockSpec(memory_space=pltpu.HBM)] * 4,
        out_specs=[vm] * (GROUPS + 1),
        scratch_shapes=[pltpu.VMEM(v.shape, v.dtype) for v in operands]
        + [pltpu.SemaphoreType.DMA((len(operands),))],
        compiler_params=SMALL,
        name="select",
    )(*operands)


def up_kernel(parts, gate_parts, first_gate, *refs):
    xs, gate_refs = refs[:parts], refs[parts : parts + gate_parts]
    up, hid, x, acc = refs[parts + gate_parts :]
    step = pl.program_id(0)
    chunk = x.shape[1] // STEPS
    per_node, _, part = up.shape

    @pl.when(step == 0)
    def _():
        at = 0
        for p in xs:
            x[at : at + p.shape[0], :] = p[:, : x.shape[1]]
            at += p.shape[0]

    cols = x[:, pl.ds(pl.multiple_of(step * chunk, 128), chunk)]
    weight = jnp.concatenate([up[e] for e in range(per_node)], axis=1)
    value = jnp.dot(cols, weight, preferred_element_type=F32)

    @pl.when(step == 0)
    def _():
        acc[...] = value

    @pl.when(step > 0)
    def _():
        acc[...] += value

    @pl.when(step == STEPS - 1)
    def _():
        gates = jnp.concatenate([r[...] for r in gate_refs], axis=0).astype(F32)
        for e in range(per_node):
            piece = slice(e * part, (e + 1) * part)
            v = acc[:, piece]
            hid[:, piece] = (v / (1.0 + jnp.exp(-v)) * gates[:, first_gate + e : first_gate + e + 1]).astype(BF)


def cost(rows, width, units):
    return pl.CostEstimate(
        flops=2 * rows * width * units,
        transcendentals=0,
        bytes_accessed=2 * (width * units + rows * width + rows * units),
    )


def up_project(parts, gate_parts, first_gate, up):
    per_node, width, part = up.shape
    units = per_node * part
    rows = sum(p.shape[0] for p in parts)
    return pl.pallas_call(
        functools.partial(up_kernel, len(parts), len(gate_parts), first_gate),
        grid=(STEPS,),
        out_shape=jax.ShapeDtypeStruct((rows, units), BF),
        in_specs=[pl.BlockSpec(p.shape, lambda i: (0, 0)) for p in parts]
        + [pl.BlockSpec((p.shape[0], LANES), lambda i: (0, width // LANES)) for p in gate_parts]
        + [pl.BlockSpec((per_node, width // STEPS, part), lambda i: (0, i, 0))],
        out_specs=pl.BlockSpec((rows, units), lambda i: (0, 0)),
        scratch_shapes=[pltpu.VMEM((rows, width), BF), pltpu.VMEM((rows, units), F32)],
        compiler_params=LARGE,
        cost_estimate=cost(rows, width, units),
        name="up",
    )(*parts, *gate_parts, up)


def down_kernel(hid, down, *outs):
    per_node, part, chunk = down.shape
    weight = down[...].reshape(per_node * part, chunk)
    value = jnp.dot(hid[...], weight, preferred_element_type=F32).astype(BF)
    at = 0
    for o in outs:
        o[...] = value[at : at + o.shape[0]]
        at += o.shape[0]


def down_project(hid, down, sizes):
    per_node, part, width = down.shape
    rows, units = hid.shape
    chunk = width // STEPS
    return pl.pallas_call(
        down_kernel,
        grid=(STEPS,),
        out_shape=[jax.ShapeDtypeStruct((s, width), BF) for s in sizes],
        in_specs=[
            pl.BlockSpec((rows, units), lambda i: (0, 0)),
            pl.BlockSpec((per_node, part, chunk), lambda i: (0, 0, i)),
        ],
        out_specs=[pl.BlockSpec((s, chunk), lambda i: (0, i)) for s in sizes],
        compiler_params=LARGE,
        cost_estimate=cost(rows, width, units),
        name="down",
    )(hid, down)


def shift(value, by):
    size = lax.axis_size("local")
    return lax.ppermute(value, "local", [(i, (i + by) % size) for i in range(size)])


def to_nodes(value, nodes):
    rows, width = value.shape
    pieces = value.reshape(nodes, rows // nodes, 2, width // 2)
    swapped = lax.all_to_all(pieces, "node", split_axis=0, concat_axis=0, tiled=True)
    return swapped.reshape(rows, width)


def add(*values):
    total = values[0].astype(F32)
    for v in values[1:]:
        total = total + v.astype(F32)
    return total.astype(BF)


def body(tokens, node_ids, expert_ids, gate_weights, up_weight, down_weight):
    nodes = lax.axis_size("node")
    place, *groups = select(
        tokens, node_ids, expert_ids, gate_weights, nodes, up_weight.shape[0]
    )
    half = groups[0].shape[0] // 2
    gathered = []
    for g, sent in enumerate(groups):
        own = to_nodes(sent, nodes)
        used = up_weight.shape[1] + (LANES if g == 0 else 0)
        top, low = own[:half, :used], own[half:, :used]
        right_top, left_low = shift(top, 1), shift(low, -1)
        right_low, left_top = shift(low, 1), shift(top, -1)
        far_a, far_b = shift(right_top, 1), shift(left_low, -1)
        parts = (top, low, right_top, right_low, left_top, left_low, far_a, far_b)
        gathered.append(parts)
    returned = []
    for g, parts in enumerate(gathered):
        hid = up_project(parts, gathered[0], g * up_weight.shape[0], up_weight)
        own, right, left, far_a, far_b = down_project(hid, down_weight, [2 * half] * 3 + [half] * 2)
        in_a, in_b = shift(far_a, 1), shift(far_b, -1)
        late_left, late_right = shift(left[half:], 1), shift(right[:half], -1)
        soon_left = shift(add(left[:half], in_a), 1)
        soon_right = shift(add(right[half:], in_b), -1)
        total = jnp.concatenate(
            [add(own[:half], soon_left, late_right), add(own[half:], late_left, soon_right)], axis=0
        )
        returned.append(to_nodes(total, nodes))
    combined = lax.dot_general(
        place,
        jnp.concatenate(returned, axis=0),
        (((0,), (0,)), ((), ())),
        preferred_element_type=F32,
    )
    return combined.astype(BF)


def solution(mesh):
    in_specs = (
        P(("node", "local"), None),
        P(("node", "local"), None),
        P(("node", "local"), None),
        P(("node", "local"), None),
        P("node", None, "local"),
        P("node", "local", None),
    )
    out_specs = P(("node", "local"), None)

    return jax.shard_map(body, mesh=mesh, in_specs=in_specs, out_specs=out_specs, check_vma=False)
```
